32 devices in a mesh: mkt: 4 (over z), draw: 4 (over y, core), nest: 2 (over x).
Axes of the slice: x: 2, y: 2, z: 4, core: 2. Of those that a mesh axis runs over, the one named last changes fastest.
Arguments:
- features: bfloat16 [32, 512, 128], P(None, 'mkt'), may hold values from -1.5 to 1.5
- taste_draws: bfloat16 [128, 32, 512], P('mkt', None, 'draw'), may hold values from -4 to 4
- taste_scale: float32 [32], replicated, may hold values from 0.2 to 1
- nest_param: float32 [16], P('nest'), may hold values from 0.3 to 0.95
- members: int32 [16, 48], P('nest'), may hold values from -1 to 511, as said below
- log_share: float32 [512, 128], P('mkt'), may hold values from -10 to -7
Outputs:
- mean_utility: float32 [128, 768], P('mkt', 'nest')
- model_share: float32 [128, 768], P('mkt', 'nest')
The draws below stay inside these ranges and needn't reach their ends.
Inputs may be any that keep to these rules, and one draw needn't show every extreme that they name: `members`: every product id 0 to 511 stands in exactly one slot; in each nest's row the ids fill the first slots and -1 fills the rest; each nest holds at least 16 products, and some nest fills all 48 slots.
All inputs are finite; a program needn't handle non-finite values.
Results may differ from the reference program's by a relative error of at most 0.0013.
The reference program's roundings to bfloat16 on the way count: a program that leaves them out, or rounds other values in their place, can miss the bound.
Values may be sent and summed in bfloat16 or wider, within the bound.
A program may use at most 64 MiB of HBM per device.

```python
import math
import jax
import jax.numpy as jnp
from jax import lax

K = 32
J = 512
G = 16
SLOTS = 48
MARKETS = 128
DRAWS = 512
ITERS = 3


def draw_members(key, part):
    first_key, second_key, third_key = jax.random.split(key, 3)
    baseline_size = J // G
    half_size = baseline_size // 2
    shifts = jax.random.randint(first_key, (G // 2,), 0, half_size + 1).astype(jnp.int32)
    shifts = shifts.at[0].set(half_size)
    sizes = jnp.stack([baseline_size + shifts, baseline_size - shifts], axis=1).reshape(G)
    nest_order = jax.random.permutation(second_key, G)
    sizes = sizes[nest_order].astype(jnp.int32)
    offsets = (jnp.cumsum(sizes) - sizes).astype(jnp.int32)
    products = jax.random.permutation(third_key, J).astype(jnp.int32)
    slot_index = jnp.arange(SLOTS, dtype=jnp.int32)[None, :]
    position = jnp.minimum(offsets[:, None] + slot_index, J - 1)
    return jnp.where(slot_index < sizes[:, None], products[position], -1).astype(jnp.int32)


def steps_of(own_key, shape, cuts, least, top_value):
    loudness, own = 1.0, jax.random.fold_in(own_key, 6)
    for dim, blocks in cuts:
        draws = jnp.exp(jax.random.uniform(jax.random.fold_in(own, dim), (blocks,), jnp.float32, least / len(cuts), top_value / len(cuts)))
        loudness = loudness * jnp.repeat(draws, shape[dim] // blocks).reshape([-1 if axis == dim else 1 for axis in range(len(shape))])
    return loudness


def noise(stream_key, extent, deviation, bound, shards=(), kind=jnp.bfloat16):
    loudness = steps_of(stream_key, extent, shards, -0.22, 0.18) if shards else 1.0
    values = jax.random.normal(stream_key, extent, jnp.float32) * deviation * loudness
    return jnp.minimum(jnp.maximum(values, -bound), bound).astype(kind)


def setup_inputs(seed: int = 0) -> dict:
    seeds = jax.random.split(jax.random.key(seed), 7)
    return {
        "features": noise(seeds[0], (K, J, MARKETS), 0.25, 1.5, ((1, 4),)),
        "taste_draws": noise(seeds[1], (MARKETS, K, DRAWS), 1.0, 4.0, ((0, 4), (2, 4))),
        "taste_scale": jnp.clip(jax.random.uniform(seeds[2], (K,), jnp.float32, 0.2, 1.0), 0.2, 1.0),
        "nest_param": jnp.clip(jnp.exp(math.log(0.95) - 1.1526795 * jax.random.uniform(seeds[3], (G,), jnp.float32) ** steps_of(seeds[3], (G,), ((0, 2),), -0.2, 0.2)), 0.3, 0.95),
        "members": draw_members(jax.random.fold_in(seeds[6], 71), 0),
        "log_share": jnp.clip(-10.0 + 3.0 * jax.random.uniform(seeds[5], (J, MARKETS), jnp.float32) ** steps_of(seeds[5], (J, MARKETS), ((0, 4),), -0.2, 0.2), -10.0, -7.0),
    }


def revise(value_slot, slot_share, target, nest_rate, occupied):
    safe_share = jnp.where(occupied[None, :], slot_share, 1.0)
    moved_value = value_slot + (1.0 - nest_rate)[None, :] * (target - jnp.log(safe_share))
    return jnp.where(occupied[None, :], moved_value, 0.0)


def reference(features, taste_draws, taste_scale, nest_param, members, log_share):
    columns = G * SLOTS
    product_ids = members.reshape(columns).astype(jnp.int32)
    occupied = product_ids >= 0
    safe_ids = jnp.maximum(product_ids, 0).astype(jnp.int32)
    live_flag = occupied.astype(jnp.float32)
    picked = jnp.take(features, safe_ids, axis=1)
    slot_features = jnp.where(occupied[None, :, None], picked, jnp.zeros((), jnp.bfloat16))
    slot_features = jnp.transpose(slot_features, (2, 0, 1))
    slot_log = jnp.transpose(jnp.take(log_share, safe_ids, axis=0), (1, 0))
    outside = 1.0 - jnp.sum(jnp.exp(log_share), axis=0)
    start_value = jnp.where(occupied[None, :], slot_log - jnp.log(outside)[:, None], 0.0)
    taste_matrix = (taste_scale[None, :, None] * taste_draws.astype(jnp.float32)).astype(jnp.bfloat16)
    nest_rate = jnp.repeat(nest_param, SLOTS)
    block_size = math.gcd(MARKETS, 8)
    block_count = MARKETS // block_size

    def market_block(operands):
        char_block, taste_block, value_block, target_block = operands
        mean_utility_part = jnp.einsum("bks,bkr->bsr", char_block.astype(jnp.float32), taste_block.astype(jnp.float32), precision=lax.Precision.HIGHEST)
        share_block = jnp.zeros_like(value_block)
        for iteration in range(ITERS):
            utility = live_flag[None, :, None] * jnp.exp((value_block[:, :, None] + mean_utility_part) / nest_rate[None, :, None])
            grouped = utility.reshape(block_size, G, SLOTS, DRAWS)
            inner_sum = jnp.sum(grouped, axis=2)
            inclusive_value = jnp.exp(nest_param[None, :, None] * jnp.log(inner_sum))
            nest_ratio = inclusive_value / (inner_sum * (1.0 + jnp.sum(inclusive_value, axis=1))[:, None, :])
            share_block = jnp.sum(grouped * nest_ratio[:, :, None, :], axis=3).reshape(block_size, columns) / DRAWS
            value_block = revise(value_block, share_block, target_block, nest_rate, occupied)
        return value_block, share_block

    operands = (slot_features.reshape(block_count, block_size, K, columns), taste_matrix.reshape(block_count, block_size, K, DRAWS), start_value.reshape(block_count, block_size, columns), slot_log.reshape(block_count, block_size, columns))
    value_out, share_out = lax.map(market_block, operands)
    return value_out.reshape(MARKETS, columns), share_out.reshape(MARKETS, columns)
```

```python
import functools
import math

import jax
import jax.numpy as jnp
from jax import lax
from jax.experimental import pallas as pl
from jax.experimental.pallas import tpu as pltpu
from jax.sharding import PartitionSpec as P

ITERS = 3
GROUP = 8
LANES = 128
LOG2E = math.log2(math.e)
EMPTY = -1e30
MESH = pl.DeviceIdType.MESH
F32 = jnp.float32
BF16 = jnp.bfloat16


def split3(x):
    hi = x.astype(BF16).astype(F32)
    rest = x - hi
    mid = rest.astype(BF16).astype(F32)
    return hi, mid, rest - mid


def kernel(
    n_nest, n_draw, total_draws,
    sx_ref, taste_ref, value0_ref, target_ref, rate_row_ref, live_row_ref, rate_col_ref, live_col_ref,
    value_ref, share_ref,
    mu_ref, u_ref, inner_ref, incl_ref, hi_ref, lo_ref, spread_ref, pick_ref, vcat_ref,
    tot_send, tot_recv, part_send, part_recv,
    tot_ssem, tot_rsem, part_ssem, part_rsem,
):
    markets, _, cols = sx_ref.shape
    draws = taste_ref.shape[2]
    nests = rate_col_ref.shape[0]
    slots = cols // nests
    chunks = markets // GROUP
    my_nest = lax.axis_index("nest")
    my_draw = lax.axis_index("draw")
    nest_peers = [lax.rem(my_nest + d, n_nest) for d in range(1, n_nest)]
    draw_peers = [lax.rem(my_draw + d, n_draw) for d in range(1, n_draw)]

    barrier = pltpu.get_barrier_semaphore()
    for peer in nest_peers:
        pl.semaphore_signal(barrier, inc=1, device_id={"nest": peer}, device_id_type=MESH)
    for peer in draw_peers:
        pl.semaphore_signal(barrier, inc=1, device_id={"draw": peer}, device_id_type=MESH)
    pl.semaphore_wait(barrier, n_nest + n_draw - 2)

    def tot_copy(it, ch, k):
        return pltpu.make_async_remote_copy(
            src_ref=tot_send.at[it, ch], dst_ref=tot_recv.at[it, ch, k],
            send_sem=tot_ssem.at[it, ch, k], recv_sem=tot_rsem.at[it, ch, k],
            device_id={"nest": nest_peers[k]}, device_id_type=MESH)

    def part_copy(it, ch, k):
        return pltpu.make_async_remote_copy(
            src_ref=part_send.at[it, ch], dst_ref=part_recv.at[it, ch, k],
            send_sem=part_ssem.at[it, ch, k], recv_sem=part_rsem.at[it, ch, k],
            device_id={"draw": draw_peers[k]}, device_id_type=MESH)

    row = lax.broadcasted_iota(jnp.int32, (LANES, draws), 0)
    lane = lax.broadcasted_iota(jnp.int32, (draws, LANES), 1)
    for i in range(GROUP):
        mine = (row == i) | (row == GROUP + i) | (row == 2 * GROUP + i)
        spread_ref[i] = jnp.where(mine, 1.0, 0.0).astype(BF16)
        pick_ref[i * draws:(i + 1) * draws, :] = jnp.where(lane == i, 1.0, 0.0).astype(BF16)

    rate_col = rate_col_ref[...]
    scale_col = LOG2E / rate_col
    rate_row = rate_row_ref[...]
    scale_row = LOG2E / rate_row
    live_row = live_row_ref[...]

    def mu_step(m, _):
        mu = lax.dot_general(sx_ref[m], taste_ref[m], (((0,), (0,)), ((), ())),
                             preferred_element_type=F32)
        mu = (mu.reshape(slots, nests, draws) * scale_col[None]).reshape(cols, draws)
        mu_ref[m] = jnp.where(live_col_ref[...] > 0.0, mu, EMPTY)
        return 0

    lax.fori_loop(0, markets, mu_step, 0)

    def utilities(it, ch, value):
        parts = split3(value * scale_row)
        stacked = jnp.concatenate(
            list(parts) + [jnp.zeros((LANES - 3 * GROUP, cols), F32)], axis=0)
        vcat_ref[...] = stacked.T.astype(BF16)

        def body(i, _):
            m = ch * GROUP + i
            shift = jnp.dot(vcat_ref[...], spread_ref[i], preferred_element_type=F32)
            u = jnp.exp2(mu_ref[m] + shift)
            u_ref[m] = u
            inner = jnp.sum(u.reshape(slots, nests, draws), axis=0)
            incl = jnp.exp(rate_col * jnp.log(inner))
            inner_ref[m] = inner
            incl_ref[m] = incl
            tot_send[it, ch, pl.ds(i, 1), :] = jnp.sum(incl, axis=0, keepdims=True)
            return 0

        lax.fori_loop(0, GROUP, body, 0)
        for k in range(n_nest - 1):
            tot_copy(it, ch, k).start()

    def shares(it, ch):
        for k in range(n_nest - 1):
            tot_copy(it, ch, k).wait_recv()

        def body(i, _):
            m = ch * GROUP + i
            total = 1.0 + tot_send[it, ch, pl.ds(i, 1), :]
            for k in range(n_nest - 1):
                total = total + tot_recv[it, ch, k, pl.ds(i, 1), :]
            ratio = incl_ref[m] / (inner_ref[m] * total)
            p = (u_ref[m].reshape(slots, nests, draws) * ratio[None]).reshape(cols, draws)
            hi = p.astype(BF16)
            at = pl.ds(pl.multiple_of(i * draws, draws), draws)
            hi_ref[:, at] = hi
            lo_ref[:, at] = (p - hi.astype(F32)).astype(BF16)
            return 0

        lax.fori_loop(0, GROUP, body, 0)
        out = jnp.dot(hi_ref[...], pick_ref[...], preferred_element_type=F32)
        out = out + jnp.dot(lo_ref[...], pick_ref[...], preferred_element_type=F32)
        part_send[it, ch] = out.T[:GROUP]
        for k in range(n_draw - 1):
            part_copy(it, ch, k).start()

    def update(it, ch):
        for k in range(n_draw - 1):
            part_copy(it, ch, k).wait_recv()
        share = part_send[it, ch]
        for k in range(n_draw - 1):
            share = share + part_recv[it, ch, k]
        share = share * (1.0 / total_draws)
        rows = pl.ds(pl.multiple_of(ch * GROUP, GROUP), GROUP)
        value = value_ref[rows, :]
        moved = value + (1.0 - rate_row) * (
            target_ref[rows, :] - jnp.log(jnp.where(live_row > 0.0, share, 1.0)))
        value = jnp.where(live_row > 0.0, moved, 0.0)
        value_ref[rows, :] = value
        if it == ITERS - 1:
            share_ref[rows, :] = share
        else:
            utilities(it + 1, ch, value)

    value_ref[...] = value0_ref[...]

    def each(fn):
        def step(ch, _):
            fn(ch)
            return 0
        lax.fori_loop(0, chunks, step, 0)

    each(lambda ch: utilities(0, ch, value_ref[pl.ds(pl.multiple_of(ch * GROUP, GROUP), GROUP), :]))
    for it in range(ITERS):
        each(functools.partial(shares, it))
        each(functools.partial(update, it))

    def drain(ch):
        for it in range(ITERS):
            for k in range(n_nest - 1):
                tot_copy(it, ch, k).wait_send()
            for k in range(n_draw - 1):
                part_copy(it, ch, k).wait_send()

    each(drain)


def iterate(sx, taste, value0, target, rate_row, live_row, rate_col, live_col, total_draws):
    markets, _, cols = sx.shape
    draws = taste.shape[2]
    nests = rate_col.shape[0]
    chunks = markets // GROUP
    n_nest = lax.axis_size("nest")
    n_draw = lax.axis_size("draw")
    vm = pl.BlockSpec(memory_space=pltpu.VMEM)
    return pl.pallas_call(
        functools.partial(kernel, n_nest, n_draw, total_draws),
        out_shape=[jax.ShapeDtypeStruct((markets, cols), F32)] * 2,
        in_specs=[vm] * 8,
        out_specs=[vm] * 2,
        scratch_shapes=[
            pltpu.VMEM((markets, cols, draws), F32),
            pltpu.VMEM((markets, cols, draws), F32),
            pltpu.VMEM((markets, nests, draws), F32),
            pltpu.VMEM((markets, nests, draws), F32),
            pltpu.VMEM((cols, GROUP * draws), BF16),
            pltpu.VMEM((cols, GROUP * draws), BF16),
            pltpu.VMEM((GROUP, LANES, draws), BF16),
            pltpu.VMEM((GROUP * draws, LANES), BF16),
            pltpu.VMEM((cols, LANES), BF16),
            pltpu.VMEM((ITERS, chunks, GROUP, draws), F32),
            pltpu.VMEM((ITERS, chunks, n_nest - 1, GROUP, draws), F32),
            pltpu.VMEM((ITERS, chunks, GROUP, cols), F32),
            pltpu.VMEM((ITERS, chunks, n_draw - 1, GROUP, cols), F32),
            pltpu.SemaphoreType.DMA((ITERS, chunks, n_nest - 1)),
            pltpu.SemaphoreType.DMA((ITERS, chunks, n_nest - 1)),
            pltpu.SemaphoreType.DMA((ITERS, chunks, n_draw - 1)),
            pltpu.SemaphoreType.DMA((ITERS, chunks, n_draw - 1)),
        ],
        compiler_params=pltpu.CompilerParams(
            collective_id=0, has_side_effects=True, vmem_limit_bytes=50 * 1024 * 1024),
        name="iterate",
    )(sx, taste, value0, target, rate_row, live_row, rate_col, live_col)


def shards(features, taste_draws, taste_scale, nest_param, members, log_share):
    market_x = lax.all_to_all(features, "mkt", split_axis=2, concat_axis=1, tiled=True)
    market_log = lax.all_to_all(log_share, "mkt", split_axis=1, concat_axis=0, tiled=True)
    markets = market_log.shape[1]
    products = market_log.shape[0]
    nests, slots = members.shape
    columns = nests * slots
    draws = taste_draws.shape[2]
    total_draws = draws * lax.axis_size("draw")
    ids = members.T.reshape(columns)
    occupied = ids >= 0
    safe_ids = jnp.maximum(ids, 0)
    onehot = (ids[None, :] == jnp.arange(products, dtype=jnp.int32)[:, None]).astype(BF16)
    sx = jnp.einsum("kjm,js->mks", market_x, onehot, preferred_element_type=F32).astype(BF16)
    target = jnp.transpose(jnp.take(market_log, safe_ids, axis=0), (1, 0))
    outside = 1.0 - jnp.sum(jnp.exp(market_log), axis=0)
    value0 = jnp.where(occupied[None, :], target - jnp.log(outside)[:, None], 0.0)
    taste = (taste_scale[None, :, None] * taste_draws.astype(F32)).astype(BF16)
    rate_row = jnp.tile(nest_param, slots)[None, :]
    live_row = occupied.astype(F32)[None, :]
    rate_col = jnp.broadcast_to(nest_param[:, None], (nests, draws))
    live_col = jnp.broadcast_to(occupied.astype(F32)[:, None], (columns, draws))
    value, share = iterate(sx, taste, value0, target, rate_row, live_row, rate_col, live_col, total_draws)

    def order(x):
        return x.reshape(markets, slots, nests).transpose(0, 2, 1).reshape(markets, columns)

    return order(value), order(share)


def solution(mesh):
    in_specs = (
        P(None, "mkt", None),
        P("mkt", None, "draw"),
        P(),
        P("nest"),
        P("nest", None),
        P("mkt", None),
    )
    out_specs = (P("mkt", "nest"), P("mkt", "nest"))
    return jax.shard_map(shards, mesh=mesh, in_specs=in_specs, out_specs=out_specs, check_vma=False)
```

```python
import functools
import math

import jax
import jax.numpy as jnp
from jax import lax
from jax.experimental import pallas as pl
from jax.experimental.pallas import tpu as pltpu
from jax.sharding import PartitionSpec as P

ITERS = 3
GROUP = 8
LANES = 128
LOG2E = math.log2(math.e)
EMPTY = -1e30
MESH = pl.DeviceIdType.MESH
F32 = jnp.float32
BF16 = jnp.bfloat16


def split3(x):
    hi = x.astype(BF16).astype(F32)
    rest = x - hi
    mid = rest.astype(BF16).astype(F32)
    return hi, mid, rest - mid


def kernel(
    n_mkt, n_nest, n_draw, total_draws,
    feat_ref, log_ref, taste_ref, scale_ref, ids_ref, param_ref,
    value_ref, share_ref,
    x_ref, logm_ref, onehot_ref, s_ref, target_ref, live_col_ref,
    mu_ref, u_ref, inner_ref, incl_ref, hi_ref, lo_ref, spread_ref, pick_ref, vcat_ref,
    tot_send, tot_recv, part_send, part_recv,
    own_sem, z_ssem, z_rsem, log_ssem, log_rsem, x_ssem, x_rsem, c_ssem, c_rsem,
    tot_ssem, tot_rsem, part_ssem, part_rsem,
):
    markets, depth, draws = taste_ref.shape
    cols = ids_ref.shape[1]
    nests = param_ref.shape[0]
    products = feat_ref.shape[3]
    slots = cols // nests
    chunks = markets // GROUP
    block = feat_ref.shape[1]
    my_mkt = lax.axis_index("mkt")
    my_nest = lax.axis_index("nest")
    my_draw = lax.axis_index("draw")
    mkt_peers = [lax.rem(my_mkt + d, n_mkt) for d in range(1, n_mkt)]
    nest_peers = [lax.rem(my_nest + d, n_nest) for d in range(1, n_nest)]
    draw_peers = [lax.rem(my_draw + d, n_draw) for d in range(1, n_draw)]
    half = lax.rem(my_draw, 2)
    partner = my_draw + 1 - 2 * half

    barrier = pltpu.get_barrier_semaphore()
    for axis, peers in (("mkt", mkt_peers), ("nest", nest_peers), ("draw", draw_peers)):
        for peer in peers:
            pl.semaphore_signal(barrier, inc=1, device_id={axis: peer}, device_id_type=MESH)

    def here(source, nest):
        return x_ref.at[source, pl.ds((2 * nest + half) * block, block)]

    def z_copy(d):
        return pltpu.make_async_remote_copy(
            src_ref=feat_ref.at[mkt_peers[d - 1]], dst_ref=here(my_mkt, my_nest),
            send_sem=z_ssem.at[d], recv_sem=z_rsem.at[d],
            device_id={"mkt": mkt_peers[d - 1]}, device_id_type=MESH)

    def log_copy(d):
        return pltpu.make_async_remote_copy(
            src_ref=log_ref.at[mkt_peers[d - 1]], dst_ref=logm_ref.at[my_mkt],
            send_sem=log_ssem.at[d], recv_sem=log_rsem.at[d],
            device_id={"mkt": mkt_peers[d - 1]}, device_id_type=MESH)

    def origin(d):
        return lax.rem(my_mkt + n_mkt - d, n_mkt)

    def own_block(d):
        return feat_ref.at[my_mkt] if d == 0 else here(origin(d), my_nest)

    def x_copy(d, k):
        return pltpu.make_async_remote_copy(
            src_ref=own_block(d), dst_ref=here(origin(d), my_nest),
            send_sem=x_ssem.at[d, k], recv_sem=x_rsem.at[d, k],
            device_id={"nest": nest_peers[k]}, device_id_type=MESH)

    def c_copy(d, k):
        nest = my_nest if k == 0 else lax.rem(my_nest + n_nest - k, n_nest)
        src = own_block(d) if k == 0 else here(origin(d), nest)
        return pltpu.make_async_remote_copy(
            src_ref=src, dst_ref=here(origin(d), nest),
            send_sem=c_ssem.at[d, k], recv_sem=c_rsem.at[d, k],
            device_id={"draw": partner}, device_id_type=MESH)

    own_x = pltpu.make_async_copy(feat_ref.at[my_mkt], here(my_mkt, my_nest), own_sem.at[0])
    own_log = pltpu.make_async_copy(log_ref.at[my_mkt], logm_ref.at[my_mkt], own_sem.at[1])
    own_x.start()
    own_log.start()
    pl.semaphore_wait(barrier, n_mkt + n_nest + n_draw - 3)
    for d in range(1, n_mkt):
        z_copy(d).start()
    for k in range(n_nest - 1):
        x_copy(0, k).start()
    c_copy(0, 0).start()
    for d in range(1, n_mkt):
        log_copy(d).start()

    def tot_copy(it, ch, k):
        return pltpu.make_async_remote_copy(
            src_ref=tot_send.at[it, ch], dst_ref=tot_recv.at[it, ch, k],
            send_sem=tot_ssem.at[it, ch, k], recv_sem=tot_rsem.at[it, ch, k],
            device_id={"nest": nest_peers[k]}, device_id_type=MESH)

    def part_copy(it, ch, k):
        return pltpu.make_async_remote_copy(
            src_ref=part_send.at[it, ch], dst_ref=part_recv.at[it, ch, k],
            send_sem=part_ssem.at[it, ch, k], recv_sem=part_rsem.at[it, ch, k],
            device_id={"draw": draw_peers[k]}, device_id_type=MESH)

    row = lax.broadcasted_iota(jnp.int32, (LANES, draws), 0)
    lane = lax.broadcasted_iota(jnp.int32, (draws, LANES), 1)
    for i in range(GROUP):
        mine = (row == i) | (row == GROUP + i) | (row == 2 * GROUP + i)
        spread_ref[i] = jnp.where(mine, 1.0, 0.0).astype(BF16)
        pick_ref[i * draws:(i + 1) * draws, :] = jnp.where(lane == i, 1.0, 0.0).astype(BF16)

    ids = ids_ref[...]
    live_row = jnp.where(ids >= 0, 1.0, 0.0)
    live_col_ref[...] = jnp.broadcast_to(live_row, (draws, cols)).T
    rate_col = jnp.broadcast_to(param_ref[...], (nests, draws))
    scale_col = LOG2E / rate_col
    rate_row = jnp.broadcast_to(rate_col[None], (slots, nests, draws)).reshape(cols, draws).T[:1]
    scale_row = LOG2E / rate_row
    product = lax.broadcasted_iota(jnp.int32, (products, cols), 0)
    for z in range(n_mkt):
        onehot_ref[z] = jnp.where(ids - z * products == product, 1.0, 0.0).astype(BF16)

    for d in range(n_mkt):
        if d == 0:
            own_x.wait()
        else:
            z_copy(d).wait_recv()
            for k in range(n_nest - 1):
                x_copy(d, k).start()
            c_copy(d, 0).start()
        for k in range(n_nest - 1):
            x_copy(d, k).wait_recv()
            c_copy(d, k + 1).start()
    for d in range(n_mkt):
        for k in range(n_nest):
            c_copy(d, k).wait_recv()
        source = origin(d)
        part = jnp.dot(x_ref[source].reshape(depth * markets, products), onehot_ref[source],
                       preferred_element_type=F32)
        for w in range(cols // LANES):
            piece = part[:, w * LANES:(w + 1) * LANES]
            if d == 0:
                s_ref[w] = piece
            else:
                s_ref[w] += piece

    def mu_step(m, _):
        rows = pl.ds(m, depth, stride=markets)
        sx = jnp.concatenate([s_ref.at[w][rows, :] for w in range(cols // LANES)], axis=1).astype(BF16)
        taste = (scale_ref[...] * taste_ref[m].astype(F32)).astype(BF16)
        mu = lax.dot_general(sx, taste, (((0,), (0,)), ((), ())), preferred_element_type=F32)
        mu = (mu.reshape(slots, nests, draws) * scale_col[None]).reshape(cols, draws)
        mu_ref[m] = jnp.where(live_col_ref[...] > 0.0, mu, EMPTY)
        return 0

    lax.fori_loop(0, markets, mu_step, 0)

    own_log.wait()
    for d in range(1, n_mkt):
        log_copy(d).wait_recv()
    target = jnp.zeros((markets, cols), F32)
    inside = jnp.zeros((markets, 1), F32)
    for z in range(n_mkt):
        logs = logm_ref[z]
        inside = inside + jnp.sum(jnp.exp(logs), axis=1, keepdims=True)
        for term in split3(logs):
            target = target + jnp.dot(term.astype(BF16), onehot_ref[z], preferred_element_type=F32)
    target_ref[...] = target
    value_ref[...] = jnp.where(live_row > 0.0, target - jnp.log(1.0 - inside), 0.0)

    def utilities(it, ch, value):
        parts = split3(value * scale_row)
        stacked = jnp.concatenate(
            list(parts) + [jnp.zeros((LANES - 3 * GROUP, cols), F32)], axis=0)
        vcat_ref[...] = stacked.T.astype(BF16)

        def body(i, _):
            m = ch * GROUP + i
            shift = jnp.dot(vcat_ref[...], spread_ref[i], preferred_element_type=F32)
            u = jnp.exp2(mu_ref[m] + shift)
            u_ref[m] = u
            inner = jnp.sum(u.reshape(slots, nests, draws), axis=0)
            incl = jnp.exp(rate_col * jnp.log(inner))
            inner_ref[m] = inner
            incl_ref[m] = incl
            tot_send[it, ch, pl.ds(i, 1), :] = jnp.sum(incl, axis=0, keepdims=True)
            return 0

        lax.fori_loop(0, GROUP, body, 0)
        for k in range(n_nest - 1):
            tot_copy(it, ch, k).start()

    def shares(it, ch):
        for k in range(n_nest - 1):
            tot_copy(it, ch, k).wait_recv()

        def body(i, _):
            m = ch * GROUP + i
            total = 1.0 + tot_send[it, ch, pl.ds(i, 1), :]
            for k in range(n_nest - 1):
                total = total + tot_recv[it, ch, k, pl.ds(i, 1), :]
            ratio = incl_ref[m] / (inner_ref[m] * total)
            p = (u_ref[m].reshape(slots, nests, draws) * ratio[None]).reshape(cols, draws)
            hi = p.astype(BF16)
            at = pl.ds(pl.multiple_of(i * draws, draws), draws)
            hi_ref[:, at] = hi
            lo_ref[:, at] = (p - hi.astype(F32)).astype(BF16)
            return 0

        lax.fori_loop(0, GROUP, body, 0)
        out = jnp.dot(hi_ref[...], pick_ref[...], preferred_element_type=F32)
        out = out + jnp.dot(lo_ref[...], pick_ref[...], preferred_element_type=F32)
        part_send[it, ch] = out.T[:GROUP]
        for k in range(n_draw - 1):
            part_copy(it, ch, k).start()

    def update(it, ch):
        for k in range(n_draw - 1):
            part_copy(it, ch, k).wait_recv()
        share = part_send[it, ch]
        for k in range(n_draw - 1):
            share = share + part_recv[it, ch, k]
        share = share * (1.0 / total_draws)
        rows = pl.ds(pl.multiple_of(ch * GROUP, GROUP), GROUP)
        value = value_ref[rows, :]
        moved = value + (1.0 - rate_row) * (
            target_ref[rows, :] - jnp.log(jnp.where(live_row > 0.0, share, 1.0)))
        value = jnp.where(live_row > 0.0, moved, 0.0)
        value_ref[rows, :] = value
        if it == ITERS - 1:
            share_ref[rows, :] = share
        else:
            utilities(it + 1, ch, value)

    def each(fn):
        def step(ch, _):
            fn(ch)
            return 0
        lax.fori_loop(0, chunks, step, 0)

    each(lambda ch: utilities(0, ch, value_ref[pl.ds(pl.multiple_of(ch * GROUP, GROUP), GROUP), :]))
    for it in range(ITERS):
        each(functools.partial(shares, it))
        each(functools.partial(update, it))

    def drain(ch):
        for it in range(ITERS):
            for k in range(n_nest - 1):
                tot_copy(it, ch, k).wait_send()
            for k in range(n_draw - 1):
                part_copy(it, ch, k).wait_send()

    each(drain)
    for d in range(n_mkt):
        if d > 0:
            z_copy(d).wait_send()
            log_copy(d).wait_send()
        for k in range(n_nest - 1):
            x_copy(d, k).wait_send()
        for k in range(n_nest):
            c_copy(d, k).wait_send()


def iterate(feat, logs, taste, scale, ids, param, total_draws):
    n_mkt = lax.axis_size("mkt")
    n_nest = lax.axis_size("nest")
    n_draw = lax.axis_size("draw")
    markets, depth, draws = taste.shape
    cols = ids.shape[1]
    nests = param.shape[0]
    products = feat.shape[3]
    chunks = markets // GROUP
    vm = pl.BlockSpec(memory_space=pltpu.VMEM)
    dma = pltpu.SemaphoreType.DMA
    return pl.pallas_call(
        functools.partial(kernel, n_mkt, n_nest, n_draw, total_draws),
        out_shape=[jax.ShapeDtypeStruct((markets, cols), F32)] * 2,
        in_specs=[vm] * 6,
        out_specs=[vm] * 2,
        scratch_shapes=[
            pltpu.VMEM((n_mkt, depth, markets, products), BF16),
            pltpu.VMEM((n_mkt, markets, products), F32),
            pltpu.VMEM((n_mkt, products, cols), BF16),
            pltpu.VMEM((cols // LANES, depth * markets, LANES), F32),
            pltpu.VMEM((markets, cols), F32),
            pltpu.VMEM((cols, draws), F32),
            pltpu.VMEM((markets, cols, draws), F32),
            pltpu.VMEM((markets, cols, draws), F32),
            pltpu.VMEM((markets, nests, draws), F32),
            pltpu.VMEM((markets, nests, draws), F32),
            pltpu.VMEM((cols, GROUP * draws), BF16),
            pltpu.VMEM((cols, GROUP * draws), BF16),
            pltpu.VMEM((GROUP, LANES, draws), BF16),
            pltpu.VMEM((GROUP * draws, LANES), BF16),
            pltpu.VMEM((cols, LANES), BF16),
            pltpu.VMEM((ITERS, chunks, GROUP, draws), F32),
            pltpu.VMEM((ITERS, chunks, n_nest - 1, GROUP, draws), F32),
            pltpu.VMEM((ITERS, chunks, GROUP, cols), F32),
            pltpu.VMEM((ITERS, chunks, n_draw - 1, GROUP, cols), F32),
            dma((2,)),
            dma((n_mkt,)), dma((n_mkt,)), dma((n_mkt,)), dma((n_mkt,)),
            dma((n_mkt, n_nest - 1)), dma((n_mkt, n_nest - 1)),
            dma((n_mkt, n_nest)), dma((n_mkt, n_nest)),
            dma((ITERS, chunks, n_nest - 1)), dma((ITERS, chunks, n_nest - 1)),
            dma((ITERS, chunks, n_draw - 1)), dma((ITERS, chunks, n_draw - 1)),
        ],
        compiler_params=pltpu.CompilerParams(
            collective_id=0, has_side_effects=True, vmem_limit_bytes=50 * 1024 * 1024),
        name="iterate",
    )(feat, logs, taste, scale, ids, param)


def shards(features, taste_draws, taste_scale, nest_param, members, log_share):
    n_mkt = lax.axis_size("mkt")
    depth, products, all_markets = features.shape
    markets = all_markets // n_mkt
    nests, slots = members.shape
    columns = nests * slots
    draws = taste_draws.shape[2]
    total_draws = draws * lax.axis_size("draw")
    block = depth // (2 * lax.axis_size("nest"))
    at = (2 * lax.axis_index("nest") + lax.rem(lax.axis_index("draw"), 2)) * block
    feat = lax.dynamic_slice_in_dim(features, at, block, axis=0)
    feat = feat.reshape(block, products, n_mkt, markets).transpose(2, 0, 3, 1)
    logs = log_share.reshape(products, n_mkt, markets).transpose(1, 2, 0)
    scale = jnp.broadcast_to(taste_scale[:, None], (depth, draws))
    ids = members.T.reshape(1, columns)
    value, share = iterate(feat, logs, taste_draws, scale, ids, nest_param[:, None], total_draws)

    def order(x):
        return x.reshape(markets, slots, nests).transpose(0, 2, 1).reshape(markets, columns)

    return order(value), order(share)


def solution(mesh):
    in_specs = (
        P(None, "mkt", None),
        P("mkt", None, "draw"),
        P(),
        P("nest"),
        P("nest", None),
        P("mkt", None),
    )
    out_specs = (P("mkt", "nest"), P("mkt", "nest"))
    return jax.shard_map(shards, mesh=mesh, in_specs=in_specs, out_specs=out_specs, check_vma=False)
```

```python
import functools
import math

import jax
import jax.numpy as jnp
from jax import lax
from jax.experimental import pallas as pl
from jax.experimental.pallas import tpu as pltpu
from jax.sharding import PartitionSpec as P

ITERS = 3
GROUP = 8
LANES = 128
PACK = 4
UNROLL = 8
LOG2E = math.log2(math.e)
EMPTY = -1e30
MESH = pl.DeviceIdType.MESH
F32 = jnp.float32
BF16 = jnp.bfloat16


def split3(x):
    hi = x.astype(BF16).astype(F32)
    rest = x - hi
    mid = rest.astype(BF16).astype(F32)
    return hi, mid, rest - mid


def kernel(
    n_mkt, n_nest, n_draw, total_draws,
    feat_ref, log_ref, taste_ref, scale_ref, ids_ref, param_ref,
    value_ref, share_ref,
    x_ref, logm_ref, onehot_ref, s_ref, target_ref, live_col_ref,
    mu_ref, u_ref, inner_ref, incl_ref, taste_ref2, shift_ref, sums_ref,
    tot_send, tot_recv, part_send, part_recv,
    own_sem, z_ssem, z_rsem, log_ssem, log_rsem, x_ssem, x_rsem, c_ssem, c_rsem,
    tot_ssem, tot_rsem, part_ssem, part_rsem,
):
    markets, depth, draws = taste_ref.shape
    cols = ids_ref.shape[1]
    nests = param_ref.shape[0]
    products = feat_ref.shape[3]
    slots = cols // nests
    chunks = markets // GROUP
    block = feat_ref.shape[1]
    my_mkt = lax.axis_index("mkt")
    my_nest = lax.axis_index("nest")
    my_draw = lax.axis_index("draw")
    mkt_peers = [lax.rem(my_mkt + d, n_mkt) for d in range(1, n_mkt)]
    nest_peers = [lax.rem(my_nest + d, n_nest) for d in range(1, n_nest)]
    draw_peers = [lax.rem(my_draw + d, n_draw) for d in range(1, n_draw)]
    half = lax.rem(my_draw, 2)
    partner = my_draw + 1 - 2 * half

    barrier = pltpu.get_barrier_semaphore()
    for axis, peers in (("mkt", mkt_peers), ("nest", nest_peers), ("draw", draw_peers)):
        for peer in peers:
            pl.semaphore_signal(barrier, inc=1, device_id={axis: peer}, device_id_type=MESH)

    def here(source, nest):
        return x_ref.at[source, pl.ds((2 * nest + half) * block, block)]

    def z_copy(d):
        return pltpu.make_async_remote_copy(
            src_ref=feat_ref.at[mkt_peers[d - 1]], dst_ref=here(my_mkt, my_nest),
            send_sem=z_ssem.at[d], recv_sem=z_rsem.at[d],
            device_id={"mkt": mkt_peers[d - 1]}, device_id_type=MESH)

    def log_copy(d):
        return pltpu.make_async_remote_copy(
            src_ref=log_ref.at[mkt_peers[d - 1]], dst_ref=logm_ref.at[my_mkt],
            send_sem=log_ssem.at[d], recv_sem=log_rsem.at[d],
            device_id={"mkt": mkt_peers[d - 1]}, device_id_type=MESH)

    def origin(d):
        return lax.rem(my_mkt + n_mkt - d, n_mkt)

    def own_block(d):
        return feat_ref.at[my_mkt] if d == 0 else here(origin(d), my_nest)

    def x_copy(d, k):
        return pltpu.make_async_remote_copy(
            src_ref=own_block(d), dst_ref=here(origin(d), my_nest),
            send_sem=x_ssem.at[d, k], recv_sem=x_rsem.at[d, k],
            device_id={"nest": nest_peers[k]}, device_id_type=MESH)

    def c_copy(d, k):
        nest = my_nest if k == 0 else lax.rem(my_nest + n_nest - k, n_nest)
        src = own_block(d) if k == 0 else here(origin(d), nest)
        return pltpu.make_async_remote_copy(
            src_ref=src, dst_ref=here(origin(d), nest),
            send_sem=c_ssem.at[d, k], recv_sem=c_rsem.at[d, k],
            device_id={"draw": partner}, device_id_type=MESH)

    own_x = pltpu.make_async_copy(feat_ref.at[my_mkt], here(my_mkt, my_nest), own_sem.at[0])
    own_log = pltpu.make_async_copy(log_ref.at[my_mkt], logm_ref.at[my_mkt], own_sem.at[1])
    own_x.start()
    own_log.start()
    pl.semaphore_wait(barrier, n_mkt + n_nest + n_draw - 3)
    for d in range(1, n_mkt):
        z_copy(d).start()
    for k in range(n_nest - 1):
        x_copy(0, k).start()
    c_copy(0, 0).start()
    for d in range(1, n_mkt):
        log_copy(d).start()

    def tot_copy(it, ch, k):
        return pltpu.make_async_remote_copy(
            src_ref=tot_send.at[it, ch], dst_ref=tot_recv.at[it, ch, k],
            send_sem=tot_ssem.at[it, ch, k], recv_sem=tot_rsem.at[it, ch, k],
            device_id={"nest": nest_peers[k]}, device_id_type=MESH)

    def part_copy(it, ch, k):
        return pltpu.make_async_remote_copy(
            src_ref=part_send.at[it, ch], dst_ref=part_recv.at[it, ch, k],
            send_sem=part_ssem.at[it, ch, k], recv_sem=part_rsem.at[it, ch, k],
            device_id={"draw": draw_peers[k]}, device_id_type=MESH)

    lane = lax.broadcasted_iota(jnp.int32, (nests, LANES), 1)
    ids = ids_ref[...]
    live_row = jnp.where(ids >= 0, 1.0, 0.0)
    live_col_ref[...] = jnp.broadcast_to(live_row, (draws, cols)).T
    rate_col = jnp.broadcast_to(param_ref[...], (nests, draws))
    scale_col = LOG2E / rate_col
    rate_row = jnp.broadcast_to(rate_col[None], (slots, nests, draws)).reshape(cols, draws).T[:1]
    scale_row = LOG2E / rate_row
    product = lax.broadcasted_iota(jnp.int32, (products, cols), 0)
    for z in range(n_mkt):
        onehot_ref[z] = jnp.where(ids - z * products == product, 1.0, 0.0).astype(BF16)

    for d in range(n_mkt):
        if d == 0:
            own_x.wait()
        else:
            z_copy(d).wait_recv()
            for k in range(n_nest - 1):
                x_copy(d, k).start()
            c_copy(d, 0).start()
        for k in range(n_nest - 1):
            x_copy(d, k).wait_recv()
            c_copy(d, k + 1).start()
    for d in range(n_mkt):
        for k in range(n_nest):
            c_copy(d, k).wait_recv()
        source = origin(d)
        part = jnp.dot(x_ref[source].reshape(depth * markets, products), onehot_ref[source],
                       preferred_element_type=F32)
        for w in range(cols // LANES):
            piece = part[:, w * LANES:(w + 1) * LANES]
            if d == 0:
                s_ref[w] = piece
            else:
                s_ref[w] += piece

    taste_ref2[...] = jnp.zeros_like(taste_ref2)

    def mu_step(step, _):
        first = step * PACK
        rows = [pl.ds(first + j, depth, stride=markets) for j in range(PACK)]
        sx = jnp.concatenate(
            [jnp.concatenate([s_ref.at[w][at, :] for at in rows], axis=0).T
             for w in range(cols // LANES)], axis=0).astype(BF16)
        for j in range(PACK):
            taste = (scale_ref[...] * taste_ref[first + j].astype(F32)).astype(BF16)
            taste_ref2[j * depth:(j + 1) * depth, j * draws:(j + 1) * draws] = taste
        mu = jnp.dot(sx, taste_ref2[...], preferred_element_type=F32)
        live = live_col_ref[...] > 0.0
        for j in range(PACK):
            part = mu[:, j * draws:(j + 1) * draws]
            part = (part.reshape(slots, nests, draws) * scale_col[None]).reshape(cols, draws)
            mu_ref[first + j] = jnp.where(live, part, EMPTY)
        return 0

    lax.fori_loop(0, markets // PACK, mu_step, 0)

    own_log.wait()
    for d in range(1, n_mkt):
        log_copy(d).wait_recv()
    target = jnp.zeros((markets, cols), F32)
    inside = jnp.zeros((markets, 1), F32)
    for z in range(n_mkt):
        logs = logm_ref[z]
        inside = inside + jnp.sum(jnp.exp(logs), axis=1, keepdims=True)
        for term in split3(logs):
            target = target + jnp.dot(term.astype(BF16), onehot_ref[z], preferred_element_type=F32)
    target_ref[...] = target
    value_ref[...] = jnp.where(live_row > 0.0, target - jnp.log(1.0 - inside), 0.0)

    def utilities(it, ch, value):
        pad = jnp.zeros((LANES - GROUP, cols), F32)
        shift_ref[...] = jnp.concatenate([value * scale_row, pad], axis=0).T

        def body(step, inner):
            inner = list(inner)
            for j in range(UNROLL):
                rows = pl.ds(pl.multiple_of((step * UNROLL + j) * nests, nests), nests)
                shift = shift_ref[rows, :]
                for i in range(GROUP):
                    m = ch * GROUP + i
                    u = jnp.exp2(mu_ref[m, rows, :] + shift[:, i:i + 1])
                    u_ref[m, rows, :] = u
                    inner[i] = inner[i] + u
            return tuple(inner)

        zero = jnp.zeros((nests, draws), F32)
        inner = lax.fori_loop(0, slots // UNROLL, body, (zero,) * GROUP)
        totals = []
        for i in range(GROUP):
            incl = jnp.exp(rate_col * jnp.log(inner[i]))
            inner_ref[ch * GROUP + i] = inner[i]
            incl_ref[ch * GROUP + i] = incl
            totals.append(jnp.sum(incl, axis=0, keepdims=True))
        tot_send[it, ch] = jnp.concatenate(totals, axis=0)
        for k in range(n_nest - 1):
            tot_copy(it, ch, k).start()

    def shares(it, ch):
        for k in range(n_nest - 1):
            tot_copy(it, ch, k).wait_recv()

        total = 1.0 + tot_send[it, ch]
        for k in range(n_nest - 1):
            total = total + tot_recv[it, ch, k]
        ratio = [incl_ref[ch * GROUP + i] / (inner_ref[ch * GROUP + i] * total[i:i + 1])
                 for i in range(GROUP)]

        def body(step, _):
            for j in range(UNROLL):
                rows = pl.ds(pl.multiple_of((step * UNROLL + j) * nests, nests), nests)
                sums = jnp.zeros((nests, LANES), F32)
                for i in range(GROUP):
                    p = u_ref[ch * GROUP + i, rows, :] * ratio[i]
                    sums = jnp.where(lane == i, jnp.sum(p, axis=1, keepdims=True), sums)
                sums_ref[rows, :] = sums
            return 0

        lax.fori_loop(0, slots // UNROLL, body, 0)
        part_send[it, ch] = sums_ref[...].T[:GROUP]
        for k in range(n_draw - 1):
            part_copy(it, ch, k).start()

    def update(it, ch):
        for k in range(n_draw - 1):
            part_copy(it, ch, k).wait_recv()
        share = part_send[it, ch]
        for k in range(n_draw - 1):
            share = share + part_recv[it, ch, k]
        share = share * (1.0 / total_draws)
        rows = pl.ds(pl.multiple_of(ch * GROUP, GROUP), GROUP)
        value = value_ref[rows, :]
        moved = value + (1.0 - rate_row) * (
            target_ref[rows, :] - jnp.log(jnp.where(live_row > 0.0, share, 1.0)))
        value = jnp.where(live_row > 0.0, moved, 0.0)
        value_ref[rows, :] = value
        if it == ITERS - 1:
            share_ref[rows, :] = share
        else:
            utilities(it + 1, ch, value)

    def each(fn):
        def step(ch, _):
            fn(ch)
            return 0
        lax.fori_loop(0, chunks, step, 0)

    each(lambda ch: utilities(0, ch, value_ref[pl.ds(pl.multiple_of(ch * GROUP, GROUP), GROUP), :]))
    for it in range(ITERS):
        each(functools.partial(shares, it))
        each(functools.partial(update, it))

    def drain(ch):
        for it in range(ITERS):
            for k in range(n_nest - 1):
                tot_copy(it, ch, k).wait_send()
            for k in range(n_draw - 1):
                part_copy(it, ch, k).wait_send()

    each(drain)
    for d in range(n_mkt):
        if d > 0:
            z_copy(d).wait_send()
            log_copy(d).wait_send()
        for k in range(n_nest - 1):
            x_copy(d, k).wait_send()
        for k in range(n_nest):
            c_copy(d, k).wait_send()


def iterate(feat, logs, taste, scale, ids, param, total_draws):
    n_mkt = lax.axis_size("mkt")
    n_nest = lax.axis_size("nest")
    n_draw = lax.axis_size("draw")
    markets, depth, draws = taste.shape
    cols = ids.shape[1]
    nests = param.shape[0]
    products = feat.shape[3]
    chunks = markets // GROUP
    vm = pl.BlockSpec(memory_space=pltpu.VMEM)
    dma = pltpu.SemaphoreType.DMA
    return pl.pallas_call(
        functools.partial(kernel, n_mkt, n_nest, n_draw, total_draws),
        out_shape=[jax.ShapeDtypeStruct((markets, cols), F32)] * 2,
        in_specs=[vm] * 6,
        out_specs=[vm] * 2,
        scratch_shapes=[
            pltpu.VMEM((n_mkt, depth, markets, products), BF16),
            pltpu.VMEM((n_mkt, markets, products), F32),
            pltpu.VMEM((n_mkt, products, cols), BF16),
            pltpu.VMEM((cols // LANES, depth * markets, LANES), F32),
            pltpu.VMEM((markets, cols), F32),
            pltpu.VMEM((cols, draws), F32),
            pltpu.VMEM((markets, cols, draws), F32),
            pltpu.VMEM((markets, cols, draws), F32),
            pltpu.VMEM((markets, nests, draws), F32),
            pltpu.VMEM((markets, nests, draws), F32),
            pltpu.VMEM((PACK * depth, PACK * draws), BF16),
            pltpu.VMEM((cols, LANES), F32),
            pltpu.VMEM((cols, LANES), F32),
            pltpu.VMEM((ITERS, chunks, GROUP, draws), F32),
            pltpu.VMEM((ITERS, chunks, n_nest - 1, GROUP, draws), F32),
            pltpu.VMEM((ITERS, chunks, GROUP, cols), F32),
            pltpu.VMEM((ITERS, chunks, n_draw - 1, GROUP, cols), F32),
            dma((2,)),
            dma((n_mkt,)), dma((n_mkt,)), dma((n_mkt,)), dma((n_mkt,)),
            dma((n_mkt, n_nest - 1)), dma((n_mkt, n_nest - 1)),
            dma((n_mkt, n_nest)), dma((n_mkt, n_nest)),
            dma((ITERS, chunks, n_nest - 1)), dma((ITERS, chunks, n_nest - 1)),
            dma((ITERS, chunks, n_draw - 1)), dma((ITERS, chunks, n_draw - 1)),
        ],
        compiler_params=pltpu.CompilerParams(
            collective_id=0, has_side_effects=True, vmem_limit_bytes=50 * 1024 * 1024),
        name="iterate",
    )(feat, logs, taste, scale, ids, param)


def shards(features, taste_draws, taste_scale, nest_param, members, log_share):
    n_mkt = lax.axis_size("mkt")
    depth, products, all_markets = features.shape
    markets = all_markets // n_mkt
    nests, slots = members.shape
    columns = nests * slots
    draws = taste_draws.shape[2]
    total_draws = draws * lax.axis_size("draw")
    block = depth // (2 * lax.axis_size("nest"))
    at = (2 * lax.axis_index("nest") + lax.rem(lax.axis_index("draw"), 2)) * block
    feat = lax.dynamic_slice_in_dim(features, at, block, axis=0)
    feat = feat.reshape(block, products, n_mkt, markets).transpose(2, 0, 3, 1)
    logs = log_share.reshape(products, n_mkt, markets).transpose(1, 2, 0)
    scale = jnp.broadcast_to(taste_scale[:, None], (depth, draws))
    ids = members.T.reshape(1, columns)
    value, share = iterate(feat, logs, taste_draws, scale, ids, nest_param[:, None], total_draws)

    def order(x):
        return x.reshape(markets, slots, nests).transpose(0, 2, 1).reshape(markets, columns)

    return order(value), order(share)


def solution(mesh):
    in_specs = (
        P(None, "mkt", None),
        P("mkt", None, "draw"),
        P(),
        P("nest"),
        P("nest", None),
        P("mkt", None),
    )
    out_specs = (P("mkt", "nest"), P("mkt", "nest"))
    return jax.shard_map(shards, mesh=mesh, in_specs=in_specs, out_specs=out_specs, check_vma=False)
```

```python
import functools
import math

import jax
import jax.numpy as jnp
from jax import lax
from jax.experimental import pallas as pl
from jax.experimental.pallas import tpu as pltpu
from jax.sharding import PartitionSpec as P

ITERS = 3
GROUP = 8
LANES = 128
PACK = 4
LOG2E = math.log2(math.e)
EMPTY = -1e30
MESH = pl.DeviceIdType.MESH
F32 = jnp.float32
BF16 = jnp.bfloat16


def split3(x):
    hi = x.astype(BF16).astype(F32)
    rest = x - hi
    mid = rest.astype(BF16).astype(F32)
    return hi, mid, rest - mid


def kernel(
    n_mkt, n_nest, n_draw, total_draws,
    feat_ref, log_ref, taste_ref, scale_ref, ids_ref, param_ref,
    value_ref, share_ref,
    x_ref, logm_ref, onehot_ref, s_ref, target_ref, live_col_ref,
    mu_ref, u_ref, inner_ref, incl_ref, taste_ref2, shift_ref, sums_ref,
    tot_send, tot_recv, part_send, part_recv,
    own_sem, z_ssem, z_rsem, log_ssem, log_rsem, x_ssem, x_rsem, c_ssem, c_rsem,
    tot_ssem, tot_rsem, part_ssem, part_rsem,
):
    markets, depth, draws = taste_ref.shape
    cols = ids_ref.shape[1]
    nests = param_ref.shape[0]
    products = feat_ref.shape[3]
    slots = cols // nests
    chunks = markets // GROUP
    block = feat_ref.shape[1]
    my_mkt = lax.axis_index("mkt")
    my_nest = lax.axis_index("nest")
    my_draw = lax.axis_index("draw")
    mkt_peers = [lax.rem(my_mkt + d, n_mkt) for d in range(1, n_mkt)]
    nest_peers = [lax.rem(my_nest + d, n_nest) for d in range(1, n_nest)]
    draw_peers = [lax.rem(my_draw + d, n_draw) for d in range(1, n_draw)]
    half = lax.rem(my_draw, 2)
    partner = my_draw + 1 - 2 * half

    barrier = pltpu.get_barrier_semaphore()
    for axis, peers in (("mkt", mkt_peers), ("nest", nest_peers), ("draw", draw_peers)):
        for peer in peers:
            pl.semaphore_signal(barrier, inc=1, device_id={axis: peer}, device_id_type=MESH)

    def here(source, nest):
        return x_ref.at[source, pl.ds((2 * nest + half) * block, block)]

    def z_copy(d):
        return pltpu.make_async_remote_copy(
            src_ref=feat_ref.at[mkt_peers[d - 1]], dst_ref=here(my_mkt, my_nest),
            send_sem=z_ssem.at[d], recv_sem=z_rsem.at[d],
            device_id={"mkt": mkt_peers[d - 1]}, device_id_type=MESH)

    def log_copy(d):
        return pltpu.make_async_remote_copy(
            src_ref=log_ref.at[mkt_peers[d - 1]], dst_ref=logm_ref.at[my_mkt],
            send_sem=log_ssem.at[d], recv_sem=log_rsem.at[d],
            device_id={"mkt": mkt_peers[d - 1]}, device_id_type=MESH)

    def origin(d):
        return lax.rem(my_mkt + n_mkt - d, n_mkt)

    def own_block(d):
        return feat_ref.at[my_mkt] if d == 0 else here(origin(d), my_nest)

    def x_copy(d, k):
        return pltpu.make_async_remote_copy(
            src_ref=own_block(d), dst_ref=here(origin(d), my_nest),
            send_sem=x_ssem.at[d, k], recv_sem=x_rsem.at[d, k],
            device_id={"nest": nest_peers[k]}, device_id_type=MESH)

    def c_copy(d, k):
        nest = my_nest if k == 0 else lax.rem(my_nest + n_nest - k, n_nest)
        src = own_block(d) if k == 0 else here(origin(d), nest)
        return pltpu.make_async_remote_copy(
            src_ref=src, dst_ref=here(origin(d), nest),
            send_sem=c_ssem.at[d, k], recv_sem=c_rsem.at[d, k],
            device_id={"draw": partner}, device_id_type=MESH)

    own_x = pltpu.make_async_copy(feat_ref.at[my_mkt], here(my_mkt, my_nest), own_sem.at[0])
    own_log = pltpu.make_async_copy(log_ref.at[my_mkt], logm_ref.at[my_mkt], own_sem.at[1])
    own_x.start()
    own_log.start()
    pl.semaphore_wait(barrier, n_mkt + n_nest + n_draw - 3)
    for d in range(1, n_mkt):
        z_copy(d).start()
    for k in range(n_nest - 1):
        x_copy(0, k).start()
    c_copy(0, 0).start()
    for d in range(1, n_mkt):
        log_copy(d).start()

    def tot_copy(it, ch, k):
        return pltpu.make_async_remote_copy(
            src_ref=tot_send.at[it, ch], dst_ref=tot_recv.at[it, ch, k],
            send_sem=tot_ssem.at[it, ch, k], recv_sem=tot_rsem.at[it, ch, k],
            device_id={"nest": nest_peers[k]}, device_id_type=MESH)

    def part_copy(it, ch, k):
        return pltpu.make_async_remote_copy(
            src_ref=part_send.at[it, ch], dst_ref=part_recv.at[it, ch, k],
            send_sem=part_ssem.at[it, ch, k], recv_sem=part_rsem.at[it, ch, k],
            device_id={"draw": draw_peers[k]}, device_id_type=MESH)

    lane = lax.broadcasted_iota(jnp.int32, (nests, LANES), 1)
    ids = ids_ref[...]
    live_row = jnp.where(ids >= 0, 1.0, 0.0)
    live_col_ref[...] = jnp.broadcast_to(live_row, (draws, cols)).T
    rate_col = jnp.broadcast_to(param_ref[...], (nests, draws))
    scale_col = LOG2E / rate_col
    rate_row = jnp.broadcast_to(rate_col[None], (slots, nests, draws)).reshape(cols, draws).T[:1]
    scale_row = LOG2E / rate_row
    product = lax.broadcasted_iota(jnp.int32, (products, cols), 0)
    for z in range(n_mkt):
        onehot_ref[z] = jnp.where(ids - z * products == product, 1.0, 0.0).astype(BF16)

    for d in range(n_mkt):
        if d == 0:
            own_x.wait()
        else:
            z_copy(d).wait_recv()
            for k in range(n_nest - 1):
                x_copy(d, k).start()
            c_copy(d, 0).start()
        for k in range(n_nest - 1):
            x_copy(d, k).wait_recv()
            c_copy(d, k + 1).start()
    for d in range(n_mkt):
        for k in range(n_nest):
            c_copy(d, k).wait_recv()
        source = origin(d)
        part = jnp.dot(x_ref[source].reshape(depth * markets, products), onehot_ref[source],
                       preferred_element_type=F32)
        for w in range(cols // LANES):
            piece = part[:, w * LANES:(w + 1) * LANES]
            if d == 0:
                s_ref[w] = piece
            else:
                s_ref[w] += piece

    taste_ref2[...] = jnp.zeros_like(taste_ref2)

    def mu_step(step, _):
        first = step * PACK
        rows = [pl.ds(first + j, depth, stride=markets) for j in range(PACK)]
        sx = jnp.concatenate(
            [jnp.concatenate([s_ref.at[w][at, :] for at in rows], axis=0).T
             for w in range(cols // LANES)], axis=0).astype(BF16)
        for j in range(PACK):
            taste = (scale_ref[...] * taste_ref[first + j].astype(F32)).astype(BF16)
            taste_ref2[j * depth:(j + 1) * depth, j * draws:(j + 1) * draws] = taste
        mu = jnp.dot(sx, taste_ref2[...], preferred_element_type=F32)
        live = live_col_ref[...] > 0.0
        for j in range(PACK):
            part = mu[:, j * draws:(j + 1) * draws]
            part = (part.reshape(slots, nests, draws) * scale_col[None]).reshape(cols, draws)
            mu_ref[first + j] = jnp.where(live, part, EMPTY)
        return 0

    lax.fori_loop(0, markets // PACK, mu_step, 0)

    own_log.wait()
    for d in range(1, n_mkt):
        log_copy(d).wait_recv()
    target = jnp.zeros((markets, cols), F32)
    inside = jnp.zeros((markets, 1), F32)
    for z in range(n_mkt):
        logs = logm_ref[z]
        inside = inside + jnp.sum(jnp.exp(logs), axis=1, keepdims=True)
        for term in split3(logs):
            target = target + jnp.dot(term.astype(BF16), onehot_ref[z], preferred_element_type=F32)
    target_ref[...] = target
    value_ref[...] = jnp.where(live_row > 0.0, target - jnp.log(1.0 - inside), 0.0)

    def utilities(it, ch, value):
        pad = jnp.zeros((LANES - GROUP, cols), F32)
        shift_ref[...] = jnp.concatenate([value * scale_row, pad], axis=0).T

        def body(step, inner):
            inner = list(inner)
            rows = [pl.ds(pl.multiple_of((step * slots + j) * nests, nests), nests)
                    for j in range(slots)]
            shifts = [shift_ref[at, :] for at in rows]
            for i in range(GROUP):
                m = ch * GROUP + i
                for at, shift in zip(rows, shifts):
                    u = jnp.exp2(mu_ref[m, at, :] + shift[:, i:i + 1])
                    u_ref[m, at, :] = u
                    inner[i] = inner[i] + u
            return tuple(inner)

        zero = jnp.zeros((nests, draws), F32)
        inner = lax.fori_loop(0, slots // slots, body, (zero,) * GROUP)
        totals = []
        for i in range(GROUP):
            incl = jnp.exp(rate_col * jnp.log(inner[i]))
            inner_ref[ch * GROUP + i] = inner[i]
            incl_ref[ch * GROUP + i] = incl
            totals.append(jnp.sum(incl, axis=0, keepdims=True))
        tot_send[it, ch] = jnp.concatenate(totals, axis=0)
        for k in range(n_nest - 1):
            tot_copy(it, ch, k).start()

    def shares(it, ch):
        for k in range(n_nest - 1):
            tot_copy(it, ch, k).wait_recv()

        total = 1.0 + tot_send[it, ch]
        for k in range(n_nest - 1):
            total = total + tot_recv[it, ch, k]
        ratio = [incl_ref[ch * GROUP + i] / (inner_ref[ch * GROUP + i] * total[i:i + 1])
                 for i in range(GROUP)]

        def body(step, _):
            for j in range(slots):
                rows = pl.ds(pl.multiple_of((step * slots + j) * nests, nests), nests)
                sums = jnp.zeros((nests, LANES), F32)
                for i in range(GROUP):
                    p = u_ref[ch * GROUP + i, rows, :] * ratio[i]
                    sums = jnp.where(lane == i, jnp.sum(p, axis=1, keepdims=True), sums)
                sums_ref[rows, :] = sums
            return 0

        lax.fori_loop(0, slots // slots, body, 0)
        part_send[it, ch] = sums_ref[...].T[:GROUP]
        for k in range(n_draw - 1):
            part_copy(it, ch, k).start()

    def update(it, ch):
        for k in range(n_draw - 1):
            part_copy(it, ch, k).wait_recv()
        share = part_send[it, ch]
        for k in range(n_draw - 1):
            share = share + part_recv[it, ch, k]
        share = share * (1.0 / total_draws)
        rows = pl.ds(pl.multiple_of(ch * GROUP, GROUP), GROUP)
        value = value_ref[rows, :]
        moved = value + (1.0 - rate_row) * (
            target_ref[rows, :] - jnp.log(jnp.where(live_row > 0.0, share, 1.0)))
        value = jnp.where(live_row > 0.0, moved, 0.0)
        value_ref[rows, :] = value
        if it == ITERS - 1:
            share_ref[rows, :] = share
        else:
            utilities(it + 1, ch, value)

    def each(fn):
        def step(ch, _):
            fn(ch)
            return 0
        lax.fori_loop(0, chunks, step, 0)

    each(lambda ch: utilities(0, ch, value_ref[pl.ds(pl.multiple_of(ch * GROUP, GROUP), GROUP), :]))
    for it in range(ITERS):
        each(functools.partial(shares, it))
        each(functools.partial(update, it))

    def drain(ch):
        for it in range(ITERS):
            for k in range(n_nest - 1):
                tot_copy(it, ch, k).wait_send()
            for k in range(n_draw - 1):
                part_copy(it, ch, k).wait_send()

    each(drain)
    for d in range(n_mkt):
        if d > 0:
            z_copy(d).wait_send()
            log_copy(d).wait_send()
        for k in range(n_nest - 1):
            x_copy(d, k).wait_send()
        for k in range(n_nest):
            c_copy(d, k).wait_send()


def iterate(feat, logs, taste, scale, ids, param, total_draws):
    n_mkt = lax.axis_size("mkt")
    n_nest = lax.axis_size("nest")
    n_draw = lax.axis_size("draw")
    markets, depth, draws = taste.shape
    cols = ids.shape[1]
    nests = param.shape[0]
    products = feat.shape[3]
    chunks = markets // GROUP
    vm = pl.BlockSpec(memory_space=pltpu.VMEM)
    dma = pltpu.SemaphoreType.DMA
    return pl.pallas_call(
        functools.partial(kernel, n_mkt, n_nest, n_draw, total_draws),
        out_shape=[jax.ShapeDtypeStruct((markets, cols), F32)] * 2,
        in_specs=[vm] * 6,
        out_specs=[vm] * 2,
        scratch_shapes=[
            pltpu.VMEM((n_mkt, depth, markets, products), BF16),
            pltpu.VMEM((n_mkt, markets, products), F32),
            pltpu.VMEM((n_mkt, products, cols), BF16),
            pltpu.VMEM((cols // LANES, depth * markets, LANES), F32),
            pltpu.VMEM((markets, cols), F32),
            pltpu.VMEM((cols, draws), F32),
            pltpu.VMEM((markets, cols, draws), F32),
            pltpu.VMEM((markets, cols, draws), F32),
            pltpu.VMEM((markets, nests, draws), F32),
            pltpu.VMEM((markets, nests, draws), F32),
            pltpu.VMEM((PACK * depth, PACK * draws), BF16),
            pltpu.VMEM((cols, LANES), F32),
            pltpu.VMEM((cols, LANES), F32),
            pltpu.VMEM((ITERS, chunks, GROUP, draws), F32),
            pltpu.VMEM((ITERS, chunks, n_nest - 1, GROUP, draws), F32),
            pltpu.VMEM((ITERS, chunks, GROUP, cols), F32),
            pltpu.VMEM((ITERS, chunks, n_draw - 1, GROUP, cols), F32),
            dma((2,)),
            dma((n_mkt,)), dma((n_mkt,)), dma((n_mkt,)), dma((n_mkt,)),
            dma((n_mkt, n_nest - 1)), dma((n_mkt, n_nest - 1)),
            dma((n_mkt, n_nest)), dma((n_mkt, n_nest)),
            dma((ITERS, chunks, n_nest - 1)), dma((ITERS, chunks, n_nest - 1)),
            dma((ITERS, chunks, n_draw - 1)), dma((ITERS, chunks, n_draw - 1)),
        ],
        compiler_params=pltpu.CompilerParams(
            collective_id=0, has_side_effects=True, vmem_limit_bytes=50 * 1024 * 1024),
        name="iterate",
    )(feat, logs, taste, scale, ids, param)


def shards(features, taste_draws, taste_scale, nest_param, members, log_share):
    n_mkt = lax.axis_size("mkt")
    depth, products, all_markets = features.shape
    markets = all_markets // n_mkt
    nests, slots = members.shape
    columns = nests * slots
    draws = taste_draws.shape[2]
    total_draws = draws * lax.axis_size("draw")
    block = depth // (2 * lax.axis_size("nest"))
    at = (2 * lax.axis_index("nest") + lax.rem(lax.axis_index("draw"), 2)) * block
    feat = lax.dynamic_slice_in_dim(features, at, block, axis=0)
    feat = feat.reshape(block, products, n_mkt, markets).transpose(2, 0, 3, 1)
    logs = log_share.reshape(products, n_mkt, markets).transpose(1, 2, 0)
    scale = jnp.broadcast_to(taste_scale[:, None], (depth, draws))
    ids = members.T.reshape(1, columns)
    value, share = iterate(feat, logs, taste_draws, scale, ids, nest_param[:, None], total_draws)

    def order(x):
        return x.reshape(markets, slots, nests).transpose(0, 2, 1).reshape(markets, columns)

    return order(value), order(share)


def solution(mesh):
    in_specs = (
        P(None, "mkt", None),
        P("mkt", None, "draw"),
        P(),
        P("nest"),
        P("nest", None),
        P("mkt", None),
    )
    out_specs = (P("mkt", "nest"), P("mkt", "nest"))
    return jax.shard_map(shards, mesh=mesh, in_specs=in_specs, out_specs=out_specs, check_vma=False)
```
